512 devices in a mesh: sample: 4 (over y), row: 8 (over x, core), col: 16 (over z).
Axes of the slice: x: 4, y: 4, z: 16, core: 2. Of those that a mesh axis runs over, the one named last changes fastest.
Arguments:
- pair: bfloat16 [3584, 896, 128], P(('sample', 'row'), 'col'), parts along dimension 0, may hold values from -6 to 6
- pair_gain: float32 [128], replicated, may hold values from 0.1 to 1.9
- bias_weight: bfloat16 [128, 16], replicated, may hold values from -0.5 to 0.5
- single: bfloat16 [3584, 384], P(('sample', 'row', 'col')), parts along dimension 0, may hold values from -50 to 50
- w_query: bfloat16 [384, 384], replicated, may hold values from -0.30618622 to 0.30618622
- w_key: bfloat16 [384, 384], replicated, may hold values from -0.30618622 to 0.30618622
- w_value: bfloat16 [384, 384], replicated, may hold values from -0.3125 to 0.3125
- w_out: bfloat16 [384, 384], replicated, may hold values from -0.3125 to 0.3125
- key_mask: int32 [3584], P(('sample', 'col')), parts along dimension 0, may hold values from 0 to 1, as said below
- out_grad: bfloat16 [3584, 384], P(('sample', 'row', 'col')), parts along dimension 0, may hold values from -6 to 6
Outputs:
- pair_grad: bfloat16 [3584, 896, 128], P(('sample', 'row'), 'col'), parts along dimension 0
- single_grad: bfloat16 [3584, 384], P(('sample', 'row', 'col')), parts along dimension 0
- query_weight_grad: float32 [1536, 384], P(('sample', 'row', 'col')), parts along dimension 0
- key_weight_grad: float32 [1536, 384], P(('sample', 'row', 'col')), parts along dimension 0
- value_weight_grad: float32 [1536, 384], P(('sample', 'row', 'col')), parts along dimension 0
- out_weight_grad: float32 [1536, 384], P(('sample', 'row', 'col')), parts along dimension 0
- bias_weight_grad: float32 [512, 16], P('sample'), parts along dimension 0
- gain_grad: float32 [512], P('sample'), parts along dimension 0
The draws below stay inside these ranges and needn't reach their ends.
There are 4 independent parts, one for each index of `sample`. The reference program is written for one: setup_inputs(seed, part) draws one part's arguments, and reference() takes and returns one part's arrays. A program takes and returns all parts, laid end to end along the dimension named above; an argument that names none is the same for every part. Nothing has to cross between parts.
Inputs may be any that keep to these rules, and one draw needn't show every extreme that they name: key_mask is 1 exactly on a prefix of the tokens whose length is a multiple of 4, at least half of 896 and at most 892, and 0 after it.
All inputs are finite; a program needn't handle non-finite values.
Results may differ from the reference program's by a relative error of at most 0.04.
Values may be sent and summed in bfloat16 or wider, within the bound.
No kernel may reach another device: no remote copies, remote signals or barrier semaphores. Data moves between devices by JAX's collectives and lax.ppermute only.
A program may use at most 64 MiB of HBM per device.

```python
import jax
import jax.numpy as jnp
from jax import lax

D = 384
PAIR = 128
HEADS = 16
HEAD = 24
PADBLOCK = 4
TOKENS = 896


def projection_pair(key):
    first_key = jax.random.fold_in(key, 7101)
    second_key = jax.random.fold_in(key, 7102)
    spread = D ** (-0.5)
    query_weight = jnp.clip(jax.random.normal(first_key, (D, D), jnp.float32), -6.0, 6.0) * spread
    noise_weight = jnp.clip(jax.random.normal(second_key, (D, D), jnp.float32), -6.0, 6.0) * spread
    key_weight = noise_weight
    return (query_weight, key_weight)


def draw_w_query(key, part):
    return projection_pair(key)[0].astype(jnp.bfloat16)


def draw_w_key(key, part):
    return projection_pair(key)[1].astype(jnp.bfloat16)


def draw_single(key, part):
    base = jnp.clip(jax.random.normal(jax.random.fold_in(key, 7201), (TOKENS, D), jnp.float32), -6.0, 6.0)
    return base.astype(jnp.bfloat16)


def draw_key_mask(key, part):
    block_count = TOKENS // PADBLOCK
    lowest = (block_count + 1) // 2
    highest_count = block_count - 1
    choices_count = highest_count - lowest + 1
    offset = jax.random.randint(jax.random.fold_in(key, 7301), (), 0, choices_count)
    part_index = jnp.asarray(part).astype(jnp.int32)
    blocks = lowest + (offset.astype(jnp.int32) + part_index) % choices_count
    live_count = blocks * PADBLOCK
    return (jnp.arange(TOKENS, dtype=jnp.int32) < live_count).astype(jnp.int32)


def levels(key, extent, pieces, smallest, high):
    factor_of = 1.0
    for dim, blocks in pieces:
        draws = jax.random.uniform(jax.random.fold_in(jax.random.fold_in(key, 6), dim), (blocks,), jnp.float32, smallest / len(pieces), high / len(pieces))
        factor_of = factor_of * jnp.repeat(jnp.exp(draws), extent[dim] // blocks).reshape((-1,) + (1,) * (len(extent) - 1 - dim))
    return factor_of


def scatter_about(key, extent, scale, most, pieces=(), kind=jnp.bfloat16):
    values = jax.random.normal(key, extent, jnp.float32) * scale
    if len(pieces) > 0:
        values = levels(key, extent, pieces, -0.22, 0.18) * values
    return jnp.clip(values, min=-most, max=most).astype(kind)


def setup_inputs(seed: int = 0, part: int = 0) -> dict:
    key_list = jax.random.split(jax.random.key(seed), 11)
    part_keys = jax.random.split(jax.random.fold_in(key_list[10], part), 11)
    pair = scatter_about(part_keys[0], (TOKENS, TOKENS, PAIR), 1.0, 6.0, ((0, 8), (1, 16)))
    pair_gain = jnp.clip(1.0 + 0.18 * jax.random.normal(key_list[1], (PAIR,), jnp.float32), 0.1, 1.9)
    bias_weight = scatter_about(key_list[2], (PAIR, HEADS), PAIR ** -0.5, 0.5)
    single = draw_single(jax.random.fold_in(jax.random.fold_in(key_list[10], part), 71), part)
    w_query = draw_w_query(jax.random.fold_in(key_list[10], 71), part)
    w_key = draw_w_key(jax.random.fold_in(key_list[10], 71), part)
    w_value = scatter_about(key_list[6], (D, D), D ** -0.5, 0.3125)
    w_out = scatter_about(key_list[7], (D, D), D ** -0.5, 0.3125)
    key_mask = draw_key_mask(jax.random.fold_in(jax.random.fold_in(key_list[10], part), 71), part)
    out_grad = scatter_about(part_keys[9], (TOKENS, D), 1.0, 6.0, ((0, 128),))
    return dict(pair=pair, pair_gain=pair_gain, bias_weight=bias_weight, single=single, w_query=w_query, w_key=w_key, w_value=w_value, w_out=w_out, key_mask=key_mask, out_grad=out_grad)


norm_eps = 1e-05
masked_score = -1000000000.0
highest = lax.Precision.HIGHEST

def project(grads, weight):
    return jnp.dot(grads, weight.astype(jnp.float32).T, precision=highest)

def transposed_product(left, right):
    return jnp.dot(left.astype(jnp.float32).T, right, precision=highest)

def reference(pair, pair_gain, bias_weight, single, w_query, w_key, w_value, w_out, key_mask, out_grad):
    f32 = jnp.float32
    bf16 = jnp.bfloat16
    tokens = single.shape[0]
    width = single.shape[1]
    score_scale = HEAD ** (-0.5)
    pair_float = pair.astype(f32)
    centred = pair_float - lax.optimization_barrier(jnp.mean(pair_float, axis=2, keepdims=True))
    inverse = lax.rsqrt(lax.optimization_barrier(jnp.mean(centred * centred, axis=2, keepdims=True)) + norm_eps)
    normed = centred * inverse
    pair_normed = (normed * pair_gain).astype(bf16)
    pair_bias = jnp.einsum('ijc,ch->hij', pair_normed.astype(f32), bias_weight.astype(f32))
    query = jnp.dot(single, w_query, preferred_element_type=f32).astype(bf16)
    key = jnp.dot(single, w_key, preferred_element_type=f32).astype(bf16)
    value = jnp.dot(single, w_value, preferred_element_type=f32).astype(bf16)
    query_heads = query.astype(f32).reshape(tokens, HEADS, HEAD)
    key_heads = key.astype(f32).reshape(tokens, HEADS, HEAD)
    value_heads = value.astype(f32).reshape(tokens, HEADS, HEAD)
    scores = jnp.einsum('ihd,jhd->hij', query_heads, key_heads) * score_scale + pair_bias
    scores = jnp.where(key_mask[None, None, :] > 0, scores, masked_score)
    row_top = lax.optimization_barrier(jnp.max(scores, axis=2, keepdims=True))
    exp_scores = jnp.exp(scores - row_top)
    probs = exp_scores / lax.optimization_barrier(jnp.sum(exp_scores, axis=2, keepdims=True))
    probs_low = probs.astype(bf16)
    attended = jnp.einsum('hij,jhd->ihd', probs_low.astype(f32), value_heads)
    attended_flat = attended.reshape(tokens, width)
    attended_low = attended_flat.astype(bf16)
    grad_att = jnp.dot(out_grad, w_out.T, preferred_element_type=f32).astype(bf16)
    grad_heads = grad_att.astype(f32).reshape(tokens, HEADS, HEAD)
    grad_probs = jnp.einsum('ihd,jhd->hij', grad_heads, value_heads)
    row_delta = jnp.einsum('ihd,ihd->hi', grad_heads, attended)
    grad_scores = probs * (grad_probs - row_delta[:, :, None])
    grad_low = grad_scores.astype(bf16).astype(f32)
    query_grad = (jnp.einsum('hij,jhd->ihd', grad_low, key_heads) * score_scale).reshape(tokens, width)
    key_grad = (jnp.einsum('hij,ihd->jhd', grad_low, query_heads) * score_scale).reshape(tokens, width)
    value_grad = jnp.einsum('hij,ihd->jhd', probs_low.astype(f32), grad_heads).reshape(tokens, width)
    single_grad = (project(query_grad, w_query) + project(key_grad, w_key) + project(value_grad, w_value)).astype(bf16)
    query_weight_grad = transposed_product(single, query_grad)
    key_weight_grad = transposed_product(single, key_grad)
    value_weight_grad = transposed_product(single, value_grad)
    out_weight_grad = jnp.dot(attended_low.T, out_grad, preferred_element_type=f32)
    grad_normed = jnp.einsum('hij,ch->ijc', grad_low, bias_weight.astype(f32))
    bias_weight_grad = jnp.einsum('ijc,hij->ch', pair_normed.astype(f32), grad_low)
    gain_grad = lax.optimization_barrier(jnp.sum(grad_normed * normed, axis=(0, 1)))
    scaled = grad_normed * pair_gain
    pair_grad = (inverse * (scaled - lax.optimization_barrier(jnp.mean(scaled, axis=2, keepdims=True)) - normed * lax.optimization_barrier(jnp.mean(scaled * normed, axis=2, keepdims=True)))).astype(bf16)
    return (pair_grad, single_grad, query_weight_grad, key_weight_grad, value_weight_grad, out_weight_grad, bias_weight_grad, gain_grad)
```

```python
import functools

import jax
import jax.numpy as jnp
from jax import lax
from jax.experimental import pallas as pl
from jax.experimental.pallas import tpu as pltpu
from jax.sharding import Mesh
from jax.sharding import PartitionSpec as P

HEADS = 16
HEAD = 24
ROW = ("row_0", "row_1")
SAMPLE_ROW = ("sample", "row_0", "row_1")
SAMPLE_ROW_COL = ("sample", "row_0", "row_1", "col")

norm_eps = 1e-05
masked_score = -1000000000.0
score_scale = HEAD ** (-0.5)
f32 = jnp.float32
bf16 = jnp.bfloat16

OWN = 7
CHUNKS = 16
SLOTS = 128
LANES = SLOTS * HEADS
KEYS = 56
ROWS = 8
EDGE = 48
WIDTH = 384
PAIR = 128


def nn(a, b):
    return lax.dot_general(a, b, (((1,), (0,)), ((), ())), preferred_element_type=f32)


def nt(a, b):
    return lax.dot_general(a, b, (((1,), (1,)), ((), ())), preferred_element_type=f32)


def tn(a, b):
    return lax.dot_general(a, b, (((0,), (0,)), ((), ())), preferred_element_type=f32)


def expander():
    slot = lax.broadcasted_iota(jnp.int32, (SLOTS, 1), 0)
    lane = lax.broadcasted_iota(jnp.int32, (1, LANES), 1) // HEADS
    return jnp.where(slot == lane, 1.0, 0.0).astype(bf16)


def own_head():
    feature = (lax.broadcasted_iota(jnp.int32, (WIDTH, 1), 0) * 2731) >> 16
    head = lax.broadcasted_iota(jnp.int32, (1, LANES), 1) % HEADS
    return feature == head


def normalized(x):
    centred = x - jnp.mean(x, axis=-1, keepdims=True)
    inverse = lax.rsqrt(jnp.mean(centred * centred, axis=-1, keepdims=True) + norm_eps)
    return centred * inverse, inverse


def bias_kernel(pair_ref, gain_ref, spread_ref, normed_ref, bias_ref):
    gain = gain_ref[...]
    parts = []
    for t in range(OWN):
        normed, _ = normalized(pair_ref[t].astype(f32))
        parts.append((normed * gain).astype(bf16))
    block = jnp.concatenate(parts, axis=1)
    normed_ref[0] = block
    bias_ref[...] = nn(block, spread_ref[...])


def query_kernel(gathered_ref, w_query_ref, w_out_ref, query_ref, grad_ref, rows_t_ref, grads_ref):
    everything = gathered_ref[...].astype(f32)
    rows = everything[:, 0:8, :].reshape(SLOTS, WIDTH)
    grads = everything[:, 8:16, :].reshape(SLOTS, WIDTH).astype(bf16)
    rows_t_ref[...] = rows.T.astype(bf16)
    grads_ref[...] = grads
    spread = expander()
    mask = own_head()
    query = nn(rows.astype(bf16), w_query_ref[...])
    grad_att = nt(grads, w_out_ref[...])
    query_ref[...] = jnp.where(mask, nn(query.T.astype(bf16), spread), 0.0).astype(bf16)
    grad_ref[...] = jnp.where(mask, nn(grad_att.T.astype(bf16), spread), 0.0).astype(bf16)


def score_kernel(
    source_ref, cols_ref, w_key_ref, w_value_ref, mask_ref, bias_ref, query_ref, grad_ref,
    exp_ref, grad_probs_ref, stats_ref, key_t_ref, value_t_ref, cols_t_ref,
):
    padded = cols_ref[source_ref[0]]
    token = lax.broadcasted_iota(jnp.int32, (KEYS, 8 * ROWS), 0)
    slot = lax.broadcasted_iota(jnp.int32, (KEYS, 8 * ROWS), 1)
    pick = jnp.where((slot // 8) * OWN + slot % 8 == token, 1.0, 0.0)
    pick = jnp.where(slot % 8 < OWN, pick, 0.0).astype(bf16)
    cols = nn(pick, padded)
    cols_t_ref[...] = cols.T.astype(bf16)
    cols = cols.astype(bf16)
    key = nn(cols, w_key_ref[...])
    value = nn(cols, w_value_ref[...])
    key_t_ref[...] = key.T.astype(bf16)
    value_t_ref[...] = value.T.astype(bf16)
    scores = nn(key.astype(bf16), query_ref[...]) * score_scale + bias_ref[...]
    scores = jnp.where(mask_ref[...] > 0, scores, masked_score)
    top = jnp.max(scores, axis=0, keepdims=True)
    exp_scores = jnp.exp(scores - top)
    grad_probs = nn(value.astype(bf16), grad_ref[...])
    exp_ref[...] = exp_scores
    grad_probs_ref[...] = grad_probs
    total = jnp.sum(exp_scores, axis=0, keepdims=True)
    product = jnp.sum(exp_scores * grad_probs, axis=0, keepdims=True)
    tiles = [
        line[:, g * 128 : (g + 1) * 128] for line in (top, total, product) for g in range(CHUNKS)
    ]
    block = jnp.concatenate(tiles, axis=0)
    for k in range(CHUNKS):
        stats_ref[k] = block


def gradient_kernel(
    all_stats_ref, stats_ref, exp_ref, grad_probs_ref, query_ref, grad_ref, key_t_ref, value_t_ref,
    cols_t_ref, rows_t_ref, grads_ref, normed_ref, w_query_ref, w_key_ref, w_value_ref, source_ref,
    low_ref, own_ref, out_ref,
):
    tops = all_stats_ref[:, 0:CHUNKS, :]
    top = jnp.max(tops, axis=0)
    weight = jnp.exp(tops - top[None])
    total = jnp.sum(all_stats_ref[:, CHUNKS : 2 * CHUNKS, :] * weight, axis=0)
    product = jnp.sum(all_stats_ref[:, 2 * CHUNKS : 3 * CHUNKS, :] * weight, axis=0)
    factor = jnp.exp(stats_ref[0, 0:CHUNKS, :] - top) / total
    delta = product / total
    probs_parts, low_parts = [], []
    for g in range(CHUNKS):
        lanes = slice(g * 128, (g + 1) * 128)
        probs = exp_ref[:, lanes] * factor[g : g + 1, :]
        low = (probs * (grad_probs_ref[:, lanes] - delta[g : g + 1, :])).astype(bf16)
        probs_parts.append(probs.astype(bf16))
        low_parts.append(low)
    probs_low = jnp.concatenate(probs_parts, axis=1)
    grad_low = jnp.concatenate(low_parts, axis=1)
    low_ref[...] = grad_low
    mask = own_head()
    spread = expander()
    key_grad = (nt(grad_low, query_ref[...]) * score_scale).astype(bf16)
    value_grad = nt(probs_low, grad_ref[...]).astype(bf16)
    query_terms = jnp.where(mask, nn(key_t_ref[...], grad_low), 0.0).astype(bf16)
    query_grad = (nt(query_terms, spread) * score_scale).T.astype(bf16)
    attended_terms = jnp.where(mask, nn(value_t_ref[...], probs_low), 0.0).astype(bf16)
    attended_t = nt(attended_terms, spread).astype(bf16)
    own_ref[...] = nt(query_grad, w_query_ref[...])
    side = nt(key_grad, w_key_ref[...]) + nt(value_grad, w_value_ref[...])
    slot = lax.broadcasted_iota(jnp.int32, (8 * ROWS, KEYS), 0)
    token = lax.broadcasted_iota(jnp.int32, (8 * ROWS, KEYS), 1)
    place = jnp.where((slot // 8) * OWN + slot % 8 == token, 1.0, 0.0)
    place = jnp.where(slot % 8 < OWN, place, 0.0).astype(bf16)
    side = nn(place, side.astype(bf16)).astype(bf16)
    products = (
        nn(rows_t_ref[...], query_grad),
        nn(cols_t_ref[...], key_grad),
        nn(cols_t_ref[...], value_grad),
        nn(attended_t, grads_ref[...]),
    )
    for w, product_of in enumerate(products):
        product_of = product_of.astype(bf16)
        for r in range(ROWS):
            out_ref[r, w * EDGE : (w + 1) * EDGE, :] = product_of[r * EDGE : (r + 1) * EDGE, :]
    stacked = jnp.concatenate(low_parts, axis=0)
    wide = tn(stacked, normed_ref[...].reshape(CHUNKS * KEYS, OWN * PAIR))
    bias_grad = wide[0:HEADS, 0:PAIR]
    for t in range(1, OWN):
        bias_grad = bias_grad + wide[t * HEADS : (t + 1) * HEADS, t * PAIR : (t + 1) * PAIR]
    tail = jnp.concatenate(
        [bias_grad[0:8], bias_grad[8:16], jnp.zeros((8, WIDTH - 2 * PAIR), f32)], axis=1
    ).astype(bf16)
    empty = jnp.zeros((8 * ROWS, WIDTH), bf16)
    for r in range(ROWS):
        out_ref[r, 4 * EDGE : 4 * EDGE + 8 * ROWS, :] = jnp.where(source_ref[0] == r, side, empty)
        out_ref[r, 4 * EDGE + 8 * ROWS :, :] = tail


def middle_kernel(half_ref, arrived_ref, own_ref, out_ref):
    filled = arrived_ref[0].astype(f32)
    for r in range(1, ROWS):
        filled = filled + arrived_ref[r].astype(f32)
    weights = filled[0 : 4 * EDGE].astype(bf16)
    row = lax.broadcasted_iota(jnp.int32, (CHUNKS * 16, 4 * EDGE), 0)
    col = lax.broadcasted_iota(jnp.int32, (CHUNKS * 16, 4 * EDGE), 1)
    inner = row % 16
    kind = inner // 3
    wanted = kind * EDGE + (row // 16) * 3 + inner % 3
    turn = jnp.where(col == wanted, 1.0, 0.0)
    turn = jnp.where(inner < 12, turn, 0.0).astype(bf16)
    spread = nn(turn, weights).astype(bf16)
    side = filled[4 * EDGE : 4 * EDGE + 8 * ROWS]
    tail = filled[4 * EDGE + 8 * ROWS :]
    for k in range(CHUNKS):
        piece = own_ref[8 * k : 8 * k + 8, :]
        low = (k % 8) * 8
        piece = piece + jnp.where(half_ref[0] == k // 8, side[low : low + 8], 0.0)
        out_ref[k, 0:16, :] = jnp.concatenate([piece, tail], axis=0).astype(bf16)
        out_ref[k, 16:32, :] = spread[16 * k : 16 * k + 16]


def last_kernel(
    arrived_ref, gain_ref, bias_weight_t_ref, single_ref, query_ref, key_ref, value_ref, out_ref,
    bias_ref, gain_grad_ref,
):
    filled = arrived_ref[0].astype(f32)
    for k in range(1, CHUNKS):
        filled = filled + arrived_ref[k].astype(f32)
    single_ref[...] = filled[0:OWN].astype(bf16)
    query_ref[...] = filled[16:19]
    key_ref[...] = filled[19:22]
    value_ref[...] = filled[22:25]
    out_ref[...] = filled[25:28]
    bias_grad = jnp.concatenate([filled[8:16, 0:PAIR], filled[8:16, PAIR : 2 * PAIR]], axis=0)
    bias_ref[...] = bias_grad.T
    gain_grad_ref[...] = (
        jnp.sum(bias_grad * bias_weight_t_ref[...].astype(f32), axis=0, keepdims=True) / gain_ref[...]
    )


def pair_kernel(pair_ref, gain_ref, spread_ref, low_ref, out_ref):
    gain = gain_ref[...]
    wide = nn(low_ref[...], spread_ref[...])
    for t in range(OWN):
        normed, inverse = normalized(pair_ref[t].astype(f32))
        scaled = wide[:, t * PAIR : (t + 1) * PAIR] * gain
        first = jnp.mean(scaled, axis=-1, keepdims=True)
        second = jnp.mean(scaled * normed, axis=-1, keepdims=True)
        out_ref[t] = (inverse * (scaled - first - normed * second)).astype(bf16)


def whole():
    return pl.BlockSpec(memory_space=pltpu.VMEM)


def scalar():
    return pl.BlockSpec(memory_space=pltpu.SMEM)


def call(kernel, outs, *args, scalars=(), flops=1 << 20):
    return pl.pallas_call(
        kernel,
        out_shape=[jax.ShapeDtypeStruct(shape, kind) for shape, kind in outs],
        in_specs=[scalar() if k in scalars else whole() for k in range(len(args))],
        out_specs=[whole() for _ in outs],
        cost_estimate=pl.CostEstimate(flops=flops, bytes_accessed=1 << 20, transcendentals=0),
    )(*args)


def to_all(array, axes, devices):
    return lax.all_to_all(
        jnp.broadcast_to(array[None], (devices, *array.shape)), axes, 0, 0, tiled=True
    )


def body(pair, pair_gain, bias_weight, single, w_query, w_key, w_value, w_out, key_mask, out_grad):
    row_index = lax.axis_index(ROW)
    col_index = lax.axis_index("col")
    source = (col_index // 2).astype(jnp.int32)
    gain = pair_gain.reshape(1, PAIR)
    held = jnp.concatenate(
        [jnp.pad(single, ((0, 1), (0, 0))), jnp.pad(out_grad, ((0, 1), (0, 0)))], axis=0
    )
    gathered = to_all(held, "col", CHUNKS)

    eye = jnp.eye(OWN, 8, dtype=bf16)
    spread = (eye[:, None, :, None] * bias_weight[None, :, None, :]).reshape(OWN * PAIR, 128)
    normed, bias = pl.pallas_call(
        bias_kernel,
        grid=(CHUNKS,),
        in_specs=[
            pl.BlockSpec((OWN, KEYS, PAIR), lambda g: (g, 0, 0)),
            pl.BlockSpec((1, PAIR), lambda g: (0, 0)),
            pl.BlockSpec((OWN * PAIR, 128), lambda g: (0, 0)),
        ],
        out_specs=[
            pl.BlockSpec((1, KEYS, OWN * PAIR), lambda g: (g, 0, 0)),
            pl.BlockSpec((KEYS, 128), lambda g: (0, g)),
        ],
        out_shape=[
            jax.ShapeDtypeStruct((CHUNKS, KEYS, OWN * PAIR), bf16),
            jax.ShapeDtypeStruct((KEYS, LANES), f32),
        ],
        cost_estimate=pl.CostEstimate(
            flops=1 << 28, bytes_accessed=1 << 22, transcendentals=0
        ),
    )(pair, gain, spread)

    half = lax.dynamic_slice_in_dim(gathered, 8 * (col_index % 2), 8, 0)[:, 0:8]
    columns = to_all(half.reshape(8 * ROWS, WIDTH), ROW, ROWS)
    query, grad, rows_t, grads = call(
        query_kernel,
        [
            ((WIDTH, LANES), bf16),
            ((WIDTH, LANES), bf16),
            ((WIDTH, SLOTS), bf16),
            ((SLOTS, WIDTH), bf16),
        ],
        gathered, w_query, w_out,
        flops=1 << 28,
    )
    exp_scores, grad_probs, stats, key_t, value_t, cols_t = call(
        score_kernel,
        [
            ((KEYS, LANES), f32),
            ((KEYS, LANES), f32),
            ((CHUNKS, 3 * CHUNKS, 128), f32),
            ((WIDTH, KEYS), bf16),
            ((WIDTH, KEYS), bf16),
            ((WIDTH, KEYS), bf16),
        ],
        source.reshape(1), columns, w_key, w_value, key_mask.reshape(KEYS, 1), bias, query, grad,
        scalars=(0,),
    )
    all_stats = lax.all_to_all(stats, "col", 0, 0, tiled=True)
    grad_low, own_side, leaving = call(
        gradient_kernel,
        [
            ((KEYS, LANES), bf16),
            ((SLOTS, WIDTH), f32),
            ((ROWS, 4 * EDGE + 8 * ROWS + 8, WIDTH), bf16),
        ],
        all_stats, stats, exp_scores, grad_probs, query, grad, key_t, value_t, cols_t, rows_t, grads,
        normed, w_query, w_key, w_value, source.reshape(1),
        scalars=(15,),
    )
    arrived = lax.all_to_all(leaving, ROW, 0, 0, tiled=True)
    pair_grad = pl.pallas_call(
        pair_kernel,
        grid=(CHUNKS,),
        in_specs=[
            pl.BlockSpec((OWN, KEYS, PAIR), lambda g: (g, 0, 0)),
            pl.BlockSpec((1, PAIR), lambda g: (0, 0)),
            pl.BlockSpec((128, OWN * PAIR), lambda g: (0, 0)),
            pl.BlockSpec((KEYS, 128), lambda g: (0, g)),
        ],
        out_specs=pl.BlockSpec((OWN, KEYS, PAIR), lambda g: (g, 0, 0)),
        out_shape=jax.ShapeDtypeStruct(pair.shape, bf16),
        cost_estimate=pl.CostEstimate(
            flops=1 << 28, bytes_accessed=1 << 22, transcendentals=0
        ),
    )(pair, gain, spread.T, grad_low)
    half_here = jnp.where(row_index == source, col_index % 2, -1).astype(jnp.int32).reshape(1)
    (going,) = call(
        middle_kernel, [((CHUNKS, 32, WIDTH), bf16)], half_here, arrived, own_side, scalars=(0,)
    )
    landed = lax.all_to_all(going, "col", 0, 0, tiled=True)
    edge = ((3, WIDTH), f32)
    single_grad, query_grad, key_grad, value_grad, out_weight_grad, bias_grad, gain_grad = call(
        last_kernel,
        [((OWN, WIDTH), bf16), edge, edge, edge, edge, ((PAIR, HEADS), f32), ((1, PAIR), f32)],
        landed, gain, bias_weight.T,
    )
    return (
        pair_grad,
        single_grad,
        query_grad,
        key_grad,
        value_grad,
        out_weight_grad,
        bias_grad,
        gain_grad.reshape(PAIR),
    )


def solution(mesh):
    split = Mesh(
        mesh.devices.reshape(mesh.shape["sample"], 4, 2, mesh.shape["col"]),
        ("sample", "row_0", "row_1", "col"),
    )
    placed = (
        P(SAMPLE_ROW, "col", None),
        P(),
        P(),
        P(SAMPLE_ROW_COL, None),
        P(),
        P(),
        P(),
        P(),
        P(("sample", "col")),
        P(SAMPLE_ROW_COL, None),
    )
    return jax.shard_map(
        body,
        mesh=split,
        in_specs=placed,
        out_specs=(
            P(SAMPLE_ROW, "col", None),
            P(SAMPLE_ROW_COL, None),
            P(SAMPLE_ROW_COL, None),
            P(SAMPLE_ROW_COL, None),
            P(SAMPLE_ROW_COL, None),
            P(SAMPLE_ROW_COL, None),
            P("sample", None),
            P("sample"),
        ),
        check_vma=False,
    )
```
